1024 devices in a mesh: seq: 128 (over y_hi, z, x), tp: 8 (over y_lo, core).
Axes of the slice: x: 8, y: 8 (y_hi: 2, y_lo: 4; y = y_hi * 4 + y_lo), z: 8, core: 2. Of those that a mesh axis runs over, the one named last changes fastest.
Arguments:
- query_rows: bfloat16 [24576, 4096], P('seq', 'tp'), may hold values from -120 to 120
- key_rows: bfloat16 [24576, 1024], P('seq', 'tp'), may hold values from -6 to 6
- value_rows: bfloat16 [24576, 1024], P('seq', 'tp'), may hold values from -6 to 6
- document_ids: int32 [24576], replicated, may hold values from 0 to 20, never falling along the last dimension, each value on 1 to 2304 neighbouring positions
- output_weight: bfloat16 [4096, 8192], P('tp'), may hold values from -0.09375 to 0.09375
Outputs:
- attended: bfloat16 [24576, 8192], P(('seq', 'tp'))
The draws below stay inside these ranges and needn't reach their ends.
Inputs may be any that keep to these rules, and one draw needn't show every extreme that they name: `document_ids`: never falling along the sequence; every document holds at most 2304 tokens, and one holds exactly 2304.
All inputs are finite; a program needn't handle non-finite values.
Results may differ from the reference program's by a relative error of at most 0.014.
Values may be sent and summed in bfloat16 or wider, within the bound.
A program may use at most 32 MiB of HBM per device.

```python
import math
import jax
import jax.numpy as jnp
import numpy as np
from jax import lax

D = 8192
HEADS = 32
KV = 8
HD = 128
TOK_DEV = 192
SEQ = 24576
MAXDOC = 2304
N_TP = 8


def query_key_pair(key):
    key_query, key_keys = jax.random.split(key, 2)
    keys_drawn = jnp.clip(jax.random.normal(key_keys, (SEQ, KV * HD), jnp.float32), -6.0, 6.0)
    queries = jnp.clip(jax.random.normal(key_query, (SEQ, HEADS * HD), jnp.float32), -6.0, 6.0)
    return (queries, keys_drawn)


def draw_query_rows(key, part):
    return query_key_pair(jax.random.fold_in(key, 11))[0].astype(jnp.bfloat16)


def draw_key_rows(key, part):
    return query_key_pair(jax.random.fold_in(key, 11))[1].astype(jnp.bfloat16)


def level_of(own_key, dims, cuts, least, top_value):
    def one(dim, shards_of):
        draws = jax.random.uniform(jax.random.fold_in(jax.random.fold_in(own_key, 6), dim), (shards_of,), jnp.float32, least / len(cuts), top_value / len(cuts))
        return jnp.repeat(jnp.exp(draws), dims[dim] // shards_of).reshape((-1,) + (1,) * (len(dims) - dim - 1))

    loudness = one(*cuts[0])
    for cut in cuts[1:]:
        loudness = loudness * one(*cut)
    return loudness


def length_profile(amount, total, most, slope):
    loads = [(1 << 20) // math.isqrt(grade ** slope) + 1 for grade in range(2, amount + 1)]
    rest, counts = total - most - (amount - 1), [1] * (amount - 1)
    while rest > 0:
        free = [i for i in range(amount - 1) if counts[i] < most]
        whole, remaining = sum([loads[i] for i in free]), rest
        for i in free:
            addition = min(most - counts[i], max(1, remaining * loads[i] // whole), rest)
            counts[i] = counts[i] + addition
            rest = rest - addition
    return np.array([most] + counts)


def ragged(key, amount, total, most, skew):
    if amount == 2:
        one = jax.random.randint(key, (), max(1, total - most), min(most, total - 1) + 1)
        return jnp.stack([one, total - one])
    sizes = jnp.asarray(length_profile(amount, total, most, skew), jnp.int32)
    twos = (amount - 1) // 2
    donor, receiver = sizes[1:1 + 2 * twos:2], sizes[2:2 + 2 * twos:2]
    room = jnp.minimum(donor - 1, most - receiver)
    shifted = jax.random.randint(jax.random.fold_in(key, 1), (twos,), 0, 1 << 20) % (room + 1)
    sizes = sizes.at[1:1 + 2 * twos:2].set(donor - shifted).at[2:2 + 2 * twos:2].set(receiver + shifted)
    return sizes[jax.random.permutation(jax.random.fold_in(key, 2), amount)]


def bell_draw(key, shape, scale, bound, shards=(), kind=jnp.bfloat16):
    gain = level_of(key, shape, shards, -0.22, 0.18) if shards else 1.0
    entries = jax.random.normal(key, shape, jnp.float32) * scale * gain
    return jnp.minimum(jnp.maximum(entries, -bound), bound).astype(kind)


def setup_inputs(seed: int = 0) -> dict:
    keys = jax.random.split(jax.random.key(seed), 6)
    query_rows = draw_query_rows(jax.random.fold_in(keys[5], 71), 0)
    key_rows = draw_key_rows(jax.random.fold_in(keys[5], 71), 0)
    value_rows = bell_draw(keys[2], (SEQ, KV * HD), 1.0, 6.0, ((0, 128), (1, 8)))
    document_ids = jnp.searchsorted(jnp.cumsum(ragged(keys[3], 2 * SEQ // MAXDOC, SEQ, MAXDOC, 2)), jnp.arange(SEQ), side="right").astype(jnp.int32)
    output_weight = bell_draw(keys[4], (HEADS * HD, D), (HEADS * HD) ** -0.5, 0.09375, ((0, 8),))
    return dict(query_rows=query_rows, key_rows=key_rows, value_rows=value_rows, document_ids=document_ids, output_weight=output_weight)


def reference(query_rows, key_rows, value_rows, document_ids, output_weight):
    group = HEADS // KV
    query_block = 4 * TOK_DEV
    key_span = min(SEQ, MAXDOC + query_block)
    block_count = SEQ // query_block
    scaling = 1.0 / (HD ** 0.5)

    def one_block(block_index):
        query_start = (block_index * query_block).astype(jnp.int32)
        key_start = jnp.clip(query_start + query_block - key_span, 0, SEQ - key_span).astype(jnp.int32)
        queries = lax.dynamic_slice_in_dim(query_rows, query_start, query_block, 0)
        queries = queries.reshape(query_block, KV, group, HD).astype(jnp.float32)
        key_block = lax.dynamic_slice_in_dim(key_rows, key_start, key_span, 0)
        key_block = key_block.reshape(key_span, KV, HD).astype(jnp.float32)
        value_block = lax.dynamic_slice_in_dim(value_rows, key_start, key_span, 0)
        value_block = value_block.reshape(key_span, KV, HD).astype(jnp.float32)
        query_doc = lax.dynamic_slice_in_dim(document_ids, query_start, query_block, 0)
        key_doc = lax.dynamic_slice_in_dim(document_ids, key_start, key_span, 0)
        query_pos = query_start + jnp.arange(query_block, dtype=jnp.int32)
        key_pos = key_start + jnp.arange(key_span, dtype=jnp.int32)
        allowed = (key_doc[None, :] == query_doc[:, None]) & (key_pos[None, :] <= query_pos[:, None])
        scores = jnp.einsum("tkgd,ukd->kgtu", queries, key_block) * scaling
        scores = jnp.where(allowed, scores, -jnp.inf)
        row_max = jnp.max(scores, axis=-1, keepdims=True)
        exponent = jnp.exp(scores - row_max)
        denominator = jnp.sum(exponent, axis=-1)
        rounded = lax.optimization_barrier(exponent.astype(jnp.bfloat16))
        context = jnp.einsum("kgtu,ukd->kgtd", rounded.astype(jnp.float32), value_block)
        context = context / denominator[..., None]
        return context.transpose(2, 0, 1, 3).reshape(query_block, HEADS * HD)

    context = lax.map(one_block, jnp.arange(block_count, dtype=jnp.int32))
    context = context.reshape(SEQ, HEADS * HD).astype(jnp.bfloat16)
    width = HEADS * HD // N_TP
    summed = jnp.zeros((SEQ, D), jnp.float32)
    for group_index in range(N_TP):
        partial_value = jnp.dot(context[:, group_index * width:(group_index + 1) * width],
                          output_weight[group_index * width:(group_index + 1) * width],
                          preferred_element_type=jnp.float32)
        partial_value = lax.optimization_barrier(partial_value.astype(jnp.bfloat16))
        summed = summed + partial_value.astype(jnp.float32)
    return summed.astype(jnp.bfloat16)
```

```python
import functools
import math

import jax
import jax.numpy as jnp
from jax import lax
from jax.experimental import pallas as pl
from jax.experimental.pallas import tpu as pltpu
from jax.sharding import PartitionSpec as P

MESH = pl.DeviceIdType.MESH
F32 = jnp.float32
BF16 = jnp.bfloat16

T = 192
HD = 128
G = 4
L = G * T
BACK = 12
NC = 8
CW = 512
HALF = 4096
ROWS = 24
UNIT = 2 * ROWS
NEG = -1e30
SCALE = math.log2(math.e) / math.sqrt(HD)
LT = 256


def kernel(
    q_hbm, k_hbm, v_hbm, doc_ref, w_hbm, out_ref,
    kb, vb, qb, wb, start_ref, max_ref, sum_ref, acc, ctx, ctxx,
    own, psend, precv, ownx, psendx, precvx, sbuf, rbuf,
    lsem, wsem, ksend, krecv, vsend, vrecv, csem, psem, pxsem, ssem, rsem,
):
    s = lax.axis_index("seq")
    t = lax.axis_index("tp")
    x = lax.rem(s, 8)
    row = s - x
    yl = t // 2
    c = lax.rem(t, 2)
    other = lax.rem(s + 64, 128)
    edge = (yl == 0) | (yl == 3)

    def in_row(step):
        return row + lax.rem(x + step + 8, 8)

    right = (in_row(1), t)
    left = (in_row(-1), t)
    up = (lax.rem(s + 8, 128), t)
    peer = (other, t)
    twin = (s, t + 1 - 2 * c)
    yl_in = jnp.where(yl < 2, yl + 1, yl - 1)
    yl_out = jnp.where((yl == 0) | (yl == 2), 3, 0)
    inward = (s, 2 * yl_in + c)
    outward = (jnp.where(edge, other, s), 2 * yl_out + c)

    q_copies = [
        pltpu.make_async_copy(
            q_hbm.at[:, pl.ds(h * HD, HD)], qb.at[pl.ds(h * T, T), :], lsem.at[h]
        )
        for h in range(G)
    ]
    k_copy = pltpu.make_async_copy(k_hbm, kb.at[0], lsem.at[G])
    v_copy = pltpu.make_async_copy(v_hbm, vb.at[0], lsem.at[G + 1])
    w_copy = pltpu.make_async_copy(w_hbm, wb, wsem)
    k_copy.start()
    v_copy.start()
    for copy in q_copies:
        copy.start()
    w_copy.start()

    barrier = pltpu.get_barrier_semaphore()
    friends = [(in_row(m), t) for m in (1, 2, 3, -1, -2, -3)]
    friends += [up, (lax.rem(s + 120, 128), t), peer, twin, inward, outward]
    for friend in friends:
        pl.semaphore_signal(barrier, inc=1, device_id=friend, device_id_type=MESH)
    pl.semaphore_wait(barrier, len(friends))

    def kv_copy(buf, send, recv, src, dst, sem, device):
        return pltpu.make_async_remote_copy(
            src_ref=buf.at[src], dst_ref=buf.at[dst],
            send_sem=send.at[sem], recv_sem=recv.at[dst],
            device_id=device, device_id_type=MESH,
        )

    def forward(d, buf, send, recv):
        mk = functools.partial(kv_copy, buf, send, recv)
        if d <= 3:
            @pl.when(x < 7)
            def _():
                mk(d, d + 1, d + 1, right).start()
        if 8 <= d <= 11:
            @pl.when(x == 7)
            def _():
                mk(d, d - 7, d - 7, right).start()
        if d <= 4:
            mk(d, d + 8, d + 8, up).start()
        if 6 <= d <= 8:
            @pl.when((x >= 1) & (x <= d - 1))
            def _():
                mk(d, d - 1, d - 1, left).start()
        if d == 0:
            for e in (7, 6, 5):
                @pl.when(x + e <= 7)
                def _(e=e):
                    mk(0, e, e + 8, (s + e, t)).start()

    def arrive(d):
        kv_copy(kb, ksend, krecv, d, d, d, left).wait_recv()
        forward(d, kb, ksend, krecv)
        kv_copy(vb, vsend, vrecv, d, d, d, left).wait_recv()
        forward(d, vb, vsend, vrecv)

    k_copy.wait()
    forward(0, kb, ksend, krecv)
    v_copy.wait()
    forward(0, vb, vsend, vrecv)

    first = (3 * s) // 2
    odd = lax.rem(s, 2)

    def column(r):
        vals = doc_ref[pl.ds(r, 1), :].astype(F32)
        return jnp.transpose(jnp.broadcast_to(vals, (HD, HD)))

    two = jnp.concatenate([column(first), column(first + 1)], axis=0)
    qdoc = jnp.where(odd == 0, two[:T], two[HD // 2:HD // 2 + T])
    span = 21
    low = jnp.clip(first - 18, 0, T - span)

    def count(n, total):
        vals = doc_ref[pl.ds(low + n, 1), :].astype(F32)
        return total + jnp.where(vals < qdoc, 1.0, 0.0)

    counted = lax.fori_loop(0, span, count, jnp.zeros((T, HD), F32))
    counted = jnp.transpose(jnp.concatenate([counted] * G, axis=0))
    begin = jnp.sum(counted, axis=0, keepdims=True).astype(jnp.int32)
    start_ref[...] = begin + (low * HD - s * T)

    for copy in q_copies:
        copy.wait()

    max_ref[...] = jnp.full((1, L), NEG, F32)
    sum_ref[...] = jnp.zeros((1, L), F32)
    acc[...] = jnp.zeros((HD, L), F32)

    def attend(d, diagonal=False):
        keys, values = kb[d], vb[d]
        for n in range(L // LT):
            cols = pl.ds(n * LT, LT)
            scores = lax.dot_general(
                keys, qb[cols, :], (((1,), (1,)), ((), ())), preferred_element_type=F32
            )
            pos = lax.broadcasted_iota(jnp.int32, (T, LT), 0)
            allowed = pos >= start_ref[:, cols] + d * T
            if diagonal:
                lane = n * LT + lax.broadcasted_iota(jnp.int32, (1, LT), 1)
                query = lane
                for h in range(1, G):
                    query = jnp.where(lane >= h * T, lane - h * T, query)
                allowed = allowed & (pos <= query)
            scores = jnp.where(allowed, scores * SCALE, NEG)
            old = max_ref[:, cols]
            new = jnp.maximum(old, jnp.max(scores, axis=0, keepdims=True))
            expo = jnp.exp2(scores - new)
            alpha = jnp.exp2(old - new)
            max_ref[:, cols] = new
            sum_ref[:, cols] = sum_ref[:, cols] * alpha + jnp.sum(expo, axis=0, keepdims=True)
            added = lax.dot_general(
                values, expo.astype(BF16), (((0,), (0,)), ((), ())), preferred_element_type=F32
            )
            acc[:, cols] = acc[:, cols] * alpha + added

    attend(0, True)

    def attend_all(slots):
        @pl.loop(0, len(slots))
        def _(n):
            slot = slots[-1]
            for m in range(len(slots) - 1):
                slot = jnp.where(n == m, slots[m], slot)
            attend(slot)

    for slots in ((8, 1), (7, 2, 9), (6, 3, 10), (5, 4, 11), (12,)):
        for d in slots:
            arrive(d)
        attend_all(slots)

    done = jnp.transpose(acc[...] / sum_ref[...])
    for h in range(G):
        ctx[:, h * HD:(h + 1) * HD] = done[h * T:(h + 1) * T].astype(BF16)

    swap = pltpu.make_async_remote_copy(
        src_ref=ctx.at[pl.ds(pl.multiple_of(UNIT * yl_out, 16), UNIT), :], dst_ref=ctxx,
        send_sem=csem.at[0], recv_sem=csem.at[1], device_id=peer, device_id_type=MESH,
    )

    @pl.when(edge)
    def _():
        swap.start()

    w_copy.wait()

    def partner_copy(j):
        return pltpu.make_async_remote_copy(
            src_ref=psend.at[j], dst_ref=precv.at[j],
            send_sem=psem.at[0, j], recv_sem=psem.at[1, j],
            device_id=twin, device_id_type=MESH,
        )

    def partner_copy_x(j):
        return pltpu.make_async_remote_copy(
            src_ref=psendx.at[j], dst_ref=precvx.at[j],
            send_sem=pxsem.at[0, j], recv_sem=pxsem.at[1, j],
            device_id=twin, device_id_type=MESH,
        )

    def send(kind, j, slot, device):
        return pltpu.make_async_remote_copy(
            src_ref=sbuf.at[kind, j], dst_ref=rbuf.at[slot, j],
            send_sem=ssem.at[kind, j], recv_sem=rsem.at[slot, j],
            device_id=device, device_id_type=MESH,
        )

    first_slot = jnp.where(edge, 0, 2)
    second_slot = jnp.where(edge, 1, 3)
    out_slot = jnp.where(edge, 1, 0)
    far = lax.rem(yl + 2, 4)

    def products(rows, j):
        wide = [
            jnp.dot(
                rows, wb[:, pl.ds(pl.multiple_of(base + j * CW, CW), CW)],
                preferred_element_type=F32,
            )
            for base in (0, HALF)
        ]
        pieces = []
        for d in range(rows.shape[0] // UNIT):
            cores = [
                jnp.concatenate(
                    [a[d * UNIT + k * ROWS:d * UNIT + (k + 1) * ROWS] for a in wide], axis=0
                )
                for k in range(2)
            ]
            pieces.append(
                (jnp.where(c == 0, cores[0], cores[1]), jnp.where(c == 0, cores[1], cores[0]))
            )
        return pieces

    def project(j):
        for d, (mine, theirs) in enumerate(products(ctx[...], j)):
            own[d, j] = mine
            psend[j, d] = theirs.astype(BF16)
        partner_copy(j).start()

    def combine(j):
        partner_copy(j).wait_recv()
        for d in range(4):
            own[d, j] = own[d, j] + precv[j, d].astype(F32)
        sbuf[0, j] = own[far, j].astype(BF16)
        send(0, j, first_slot, inward).start()

    project(0)

    @pl.loop(1, NC)
    def _(j):
        project(j)
        combine(j - 1)

    combine(NC - 1)

    @pl.when(edge)
    def _():
        @pl.loop(0, NC)
        def _(j):
            sbuf[1, j] = own[yl_in, j].astype(BF16)
            send(1, j, second_slot, inward).start()

        swap.wait_recv()

        def project_x(j):
            ((mine, theirs),) = products(ctxx[...], j)
            ownx[j] = mine
            psendx[j] = theirs.astype(BF16)
            partner_copy_x(j).start()

        def combine_x(j):
            partner_copy_x(j).wait_recv()
            sbuf[2, j] = (ownx[j] + precvx[j].astype(F32)).astype(BF16)
            send(2, j, out_slot, outward).start()

        project_x(0)

        @pl.loop(1, NC)
        def _(j):
            project_x(j)
            combine_x(j - 1)

        combine_x(NC - 1)

    @pl.when(jnp.logical_not(edge))
    def _():
        @pl.loop(0, NC)
        def _(j):
            send(0, j, 2, inward).wait_recv()
            sbuf[2, j] = (own[yl_out, j] + rbuf[2, j].astype(F32)).astype(BF16)
            send(2, j, out_slot, outward).start()
            send(0, j, 0, inward).wait_recv()
            sbuf[1, j] = (own[yl_in, j] + rbuf[0, j].astype(F32)).astype(BF16)
            send(1, j, second_slot, inward).start()

    last_a = jnp.where(edge, 0, 1)
    last_b = jnp.where(edge, 1, 3)

    @pl.loop(0, NC)
    def _(j):
        send(0, j, last_a, inward).wait_recv()
        send(0, j, last_b, inward).wait_recv()
        total = own[yl, j] + rbuf[last_a, j].astype(F32) + rbuf[last_b, j].astype(F32)
        total = total.astype(BF16)
        out_ref[:, pl.ds(pl.multiple_of(j * CW, CW), CW)] = total[:ROWS]
        out_ref[:, pl.ds(pl.multiple_of(HALF + j * CW, CW), CW)] = total[ROWS:]

    for buf, snd, rcv in ((kb, ksend, krecv), (vb, vsend, vrecv)):
        for d in (1, 2, 3, 4, 8, 9, 10, 11, 12):
            kv_copy(buf, snd, rcv, 0, d, d, left).wait_send()
        for d in (5, 6, 7):
            @pl.when((x >= 1) & (x <= d))
            def _(d=d):
                kv_copy(buf, snd, rcv, 0, d, d, left).wait_send()

            @pl.when(x + d <= 7)
            def _(d=d):
                kv_copy(buf, snd, rcv, 0, d, d + 8, left).wait_send()

    @pl.loop(0, NC)
    def _(j):
        partner_copy(j).wait_send()
        send(0, j, first_slot, inward).wait_send()
        send(1, j, second_slot, inward).wait_send()
        send(2, j, out_slot, outward).wait_send()

    @pl.when(edge)
    def _():
        swap.wait_send()

        @pl.loop(0, NC)
        def _(j):
            partner_copy_x(j).wait_send()


def per_device(query_rows, key_rows, value_rows, document_ids, output_weight):
    any_space = pl.BlockSpec(memory_space=pl.ANY)
    vmem = pl.BlockSpec(memory_space=pltpu.VMEM)
    dma = pltpu.SemaphoreType.DMA
    return pl.pallas_call(
        kernel,
        out_shape=jax.ShapeDtypeStruct((ROWS, 2 * HALF), BF16),
        in_specs=[any_space, any_space, any_space, vmem, any_space],
        out_specs=vmem,
        scratch_shapes=[
            pltpu.VMEM((BACK + 1, T, HD), BF16),
            pltpu.VMEM((BACK + 1, T, HD), BF16),
            pltpu.VMEM((L, HD), BF16),
            pltpu.VMEM((G * HD, 2 * HALF), BF16),
            pltpu.VMEM((1, L), jnp.int32),
            pltpu.VMEM((1, L), F32),
            pltpu.VMEM((1, L), F32),
            pltpu.VMEM((HD, L), F32),
            pltpu.VMEM((T, G * HD), BF16),
            pltpu.VMEM((UNIT, G * HD), BF16),
            pltpu.VMEM((4, NC, UNIT, CW), F32),
            pltpu.VMEM((NC, 4, UNIT, CW), BF16),
            pltpu.VMEM((NC, 4, UNIT, CW), BF16),
            pltpu.VMEM((NC, UNIT, CW), F32),
            pltpu.VMEM((NC, UNIT, CW), BF16),
            pltpu.VMEM((NC, UNIT, CW), BF16),
            pltpu.VMEM((3, NC, UNIT, CW), BF16),
            pltpu.VMEM((4, NC, UNIT, CW), BF16),
            dma((G + 2,)),
            dma,
            dma((16,)),
            dma((BACK + 1,)),
            dma((16,)),
            dma((BACK + 1,)),
            dma((2,)),
            dma((2, NC)),
            dma((2, NC)),
            dma((3, NC)),
            dma((4, NC)),
        ],
        compiler_params=pltpu.CompilerParams(
            collective_id=0, has_side_effects=True, vmem_limit_bytes=56 * 1024 * 1024
        ),
        name="attend_project",
    )(query_rows, key_rows, value_rows, document_ids.reshape(T, HD), output_weight)


def solution(mesh):
    in_specs = (P("seq", "tp"), P("seq", "tp"), P("seq", "tp"), P(), P("tp", None))
    out_specs = P(("seq", "tp"), None)
    return jax.shard_map(
        per_device, mesh=mesh, in_specs=in_specs, out_specs=out_specs, check_vma=False
    )
```

```python
import functools
import math

import jax
import jax.numpy as jnp
from jax import lax
from jax.experimental import pallas as pl
from jax.experimental.pallas import tpu as pltpu
from jax.sharding import PartitionSpec as P

MESH = pl.DeviceIdType.MESH
F32 = jnp.float32
BF16 = jnp.bfloat16

T = 192
HD = 128
G = 4
L = G * T
BACK = 12
NC = 8
CW = 512
HALF = 4096
ROWS = 24
UNIT = 2 * ROWS
NEG = -1e30
PARTS = 2
PIECE = T
SLOTS = 17
TAIL = (9, 10, 11, 12)
ORDER = [(8, 1, 7, 2, 6, 3, 5, 4) + TAIL]
ORDER += [(1, 8, 2, 7, 3, 6, 4, 5) + TAIL] * 6
ORDER += [(1, 8, 2, 9, 3, 10, 4, 11, 7, 6, 5, 12)]
ORDER_Z0 = [
    (8, 1, 7, 2, 6, 9, 3, 5, 10, 4, 11, 12),
    (1, 8, 7, 9, 2, 6, 10, 3, 5, 4, 11, 12),
    (1, 2, 8, 9, 7, 10, 6, 3, 5, 11, 4, 12),
    (1, 2, 3, 8, 9, 7, 10, 6, 11, 5, 4, 12),
    (1, 2, 3, 4, 8, 9, 7, 10, 6, 11, 5, 12),
    (1, 2, 3, 4, 5, 8, 9, 7, 10, 6, 11, 12),
    (1, 2, 3, 4, 6, 5, 8, 9, 7, 10, 11, 12),
    (1, 2, 3, 4, 7, 6, 5, 8, 16, 9, 10, 11, 12),
]
SCALE = math.log2(math.e) / math.sqrt(HD)
LT = 384
WORD = 6
WORDS = 3


def packed(order):
    order = tuple(order) + (0,) * (WORD * WORDS - len(order))
    return [
        sum(d << (5 * n) for n, d in enumerate(order[w * WORD:(w + 1) * WORD]))
        for w in range(WORDS)
    ]


def kernel(
    q_hbm, k_hbm, v_hbm, doc_ref, w_hbm, out_ref,
    kvb, qb, wb, start_ref, max_ref, sum_ref, acc, ctx, ctxx,
    own, psend, precv, ownx, psendx, precvx, sbuf, rbuf,
    lsem, wsem, kvsend, kvrecv, csem, psem, pxsem, ssem, rsem,
):
    s = lax.axis_index("seq")
    t = lax.axis_index("tp")
    x = lax.rem(s, 8)
    row = s - x
    yl = t // 2
    c = lax.rem(t, 2)
    other = lax.rem(s + 64, 128)
    first_z = lax.rem(s, 64) < 8
    last_z = lax.rem(s, 64) >= 56
    across = (s >= 56) & (s < 64) & (x < 4)
    far_source = s == 55
    far_target = s == 71
    edge = (yl == 0) | (yl == 3)

    def in_row(step):
        return row + lax.rem(x + step + 8, 8)

    right = (in_row(1), t)
    left = (in_row(-1), t)
    up = (lax.rem(s + 8, 128), t)
    peer = (other, t)
    twin = (s, t + 1 - 2 * c)
    yl_in = jnp.where(yl < 2, yl + 1, yl - 1)
    yl_out = jnp.where((yl == 0) | (yl == 2), 3, 0)
    inward = (s, 2 * yl_in + c)
    outward = (jnp.where(edge, other, s), 2 * yl_out + c)

    q_copies = [
        pltpu.make_async_copy(
            q_hbm.at[:, pl.ds(h * HD, HD)], qb.at[pl.ds(h * T, T), :], lsem.at[h]
        )
        for h in range(G)
    ]
    kv_loads = [
        pltpu.make_async_copy(
            (k_hbm, v_hbm)[i], kvb.at[0, i], lsem.at[G + i],
        )
        for i in range(PARTS)
    ]
    w_copy = pltpu.make_async_copy(w_hbm, wb, wsem)
    for copy in kv_loads:
        copy.start()
    for copy in q_copies:
        copy.start()
    w_copy.start()

    barrier = pltpu.get_barrier_semaphore()
    friends = [(in_row(m), t) for m in (1, 2, -1, -2)]
    friends += [(lax.rem(s + 120, 128), t), peer, twin, inward, outward]
    for friend in friends:
        pl.semaphore_signal(barrier, inc=1, device_id=friend, device_id_type=MESH)
    far_signal = (lax.rem(s + 112, 128), t)

    @pl.when(far_target)
    def _():
        pl.semaphore_signal(barrier, inc=1, device_id=far_signal, device_id_type=MESH)

    pl.semaphore_wait(barrier, len(friends) + jnp.where(far_source, 1, 0))

    def kv_copy(src, dst, part, sem, device):
        return pltpu.make_async_remote_copy(
            src_ref=kvb.at[src, part], dst_ref=kvb.at[dst, part],
            send_sem=kvsend.at[sem, part], recv_sem=kvrecv.at[dst, part],
            device_id=device, device_id_type=MESH,
        )

    def right_sem(to):
        return jnp.where(to <= 4, to, to + 8)

    def forward(d, part):
        middle = (d >= 8) & (d <= 11)
        passing = d >= 16

        @pl.when(((x < 7) & ((d <= 3) | ((d == 4) & (x >= 4)) | (first_z & middle & (d <= x + 8)))) | ((x == 7) & (middle | passing)))
        def _():
            to = jnp.where(x < 7, d + 1, d - 7)
            kv_copy(d, to, part, right_sem(to), right).start()

        @pl.when(((d <= 4) & jnp.logical_not(last_z)) | (across & (d <= 4) & (d > jnp.maximum(x, 1 - x))))
        def _():
            kv_copy(d, d + 8, part, d + 8, up).start()

        @pl.when((d >= 6) & (d <= 8) & (x >= 1) & (x <= d - 1))
        def _():
            kv_copy(d, d - 1, part, d - 1, left).start()

    def direct(e):
        @pl.when(x + e <= 7)
        def _():
            for part in range(PARTS):
                kv_copy(0, e, part, e + 8, (s + e, t)).start()

    for part, copy in enumerate(kv_loads):
        copy.wait()

        @pl.when(x < 7)
        def _(part=part):
            kv_copy(0, 1, part, 1, right).start()

        @pl.when(s < 120)
        def _(part=part):
            kv_copy(0, 8, part, 8, up).start()

        @pl.when(far_source)
        def _(part=part):
            kv_copy(0, 16, part, 16, (s + 16, t)).start()

    direct(7)

    @pl.when(first_z)
    def _():
        direct(6)

    first = (3 * s) // 2
    odd = lax.rem(s, 2)

    def column(r):
        vals = doc_ref[pl.ds(r, 1), :].astype(F32)
        return jnp.transpose(jnp.broadcast_to(vals, (HD, HD)))

    two = jnp.concatenate([column(first), column(first + 1)], axis=0)
    qdoc = jnp.where(odd == 0, two[:T], two[HD // 2:HD // 2 + T])
    span = 21
    low = jnp.clip(first - 18, 0, T - span)

    def count(n, total):
        vals = doc_ref[pl.ds(low + n, 1), :].astype(F32)
        return total + jnp.where(vals < qdoc, 1.0, 0.0)

    counted = lax.fori_loop(0, span, count, jnp.zeros((T, HD), F32))
    counted = jnp.transpose(jnp.concatenate([counted] * G, axis=0))
    begin = jnp.sum(counted, axis=0, keepdims=True).astype(jnp.int32)
    start_ref[...] = begin + (low * HD - s * T)

    for copy in q_copies:
        copy.wait()

    max_ref[...] = jnp.full((1, L), NEG, F32)
    sum_ref[...] = jnp.zeros((1, L), F32)
    acc[...] = jnp.zeros((HD, L), F32)

    def attend(d, diagonal=False):
        keys = kvb[d, 0]
        values = kvb[d, 1]
        for n in range(L // LT):
            cols = pl.ds(n * LT, LT)
            scores = lax.dot_general(
                keys, qb[cols, :], (((1,), (1,)), ((), ())), preferred_element_type=F32
            )
            pos = lax.broadcasted_iota(jnp.int32, (T, LT), 0)
            allowed = pos >= start_ref[:, cols] + d * T
            if diagonal:
                lane = n * LT + lax.broadcasted_iota(jnp.int32, (1, LT), 1)
                query = lane
                for h in range(1, G):
                    query = jnp.where(lane >= h * T, lane - h * T, query)
                allowed = allowed & (pos <= query)
            scores = jnp.where(allowed, scores * SCALE, NEG)
            old = max_ref[:, cols]
            new = jnp.maximum(old, jnp.max(scores, axis=0, keepdims=True))
            expo = jnp.exp2(scores - new)
            alpha = jnp.exp2(old - new)
            max_ref[:, cols] = new
            sum_ref[:, cols] = sum_ref[:, cols] * alpha + jnp.sum(expo, axis=0, keepdims=True)
            added = lax.dot_general(
                values, expo.astype(BF16), (((0,), (0,)), ((), ())), preferred_element_type=F32
            )
            acc[:, cols] = acc[:, cols] * alpha + added

    attend(0, True)

    def order(index):
        word = 0
        for table, is_z0 in ((ORDER, False), (ORDER_Z0, True)):
            for place in range(8):
                here = (x == place) & (first_z if is_z0 else jnp.logical_not(first_z))
                word = jnp.where(here, packed(table[place])[index], word)
        return word

    words = [order(index) for index in range(WORDS)]

    @pl.loop(0, WORD * WORDS)
    def _(n):
        word = jnp.where(n < WORD, words[0], jnp.where(n < 2 * WORD, words[1], words[2]))
        d = lax.shift_right_logical(word, 5 * lax.rem(n, WORD)) & 31
        there = (d > 0) & (d <= s)

        @pl.when(there)
        def _():
            for part in range(PARTS):
                kv_copy(d, d, part, d, left).wait_recv()
                forward(d, part)

        @pl.when((n == 1) & jnp.logical_not(first_z))
        def _():
            direct(6)

        @pl.when(there & (d <= BACK))
        def _():
            attend(d)

    done = jnp.transpose(acc[...] / sum_ref[...])
    for h in range(G):
        ctx[:, h * HD:(h + 1) * HD] = done[h * T:(h + 1) * T].astype(BF16)

    swap = pltpu.make_async_remote_copy(
        src_ref=ctx.at[pl.ds(pl.multiple_of(UNIT * yl_out, 16), UNIT), :], dst_ref=ctxx,
        send_sem=csem.at[0], recv_sem=csem.at[1], device_id=peer, device_id_type=MESH,
    )

    @pl.when(edge)
    def _():
        swap.start()

    w_copy.wait()

    def partner_copy(j):
        return pltpu.make_async_remote_copy(
            src_ref=psend.at[j], dst_ref=precv.at[j],
            send_sem=psem.at[0, j], recv_sem=psem.at[1, j],
            device_id=twin, device_id_type=MESH,
        )

    def partner_copy_x(j):
        return pltpu.make_async_remote_copy(
            src_ref=psendx.at[j], dst_ref=precvx.at[j],
            send_sem=pxsem.at[0, j], recv_sem=pxsem.at[1, j],
            device_id=twin, device_id_type=MESH,
        )

    def send(kind, j, slot, device):
        return pltpu.make_async_remote_copy(
            src_ref=sbuf.at[kind, j], dst_ref=rbuf.at[slot, j],
            send_sem=ssem.at[kind, j], recv_sem=rsem.at[slot, j],
            device_id=device, device_id_type=MESH,
        )

    first_slot = jnp.where(edge, 0, 2)
    second_slot = jnp.where(edge, 1, 3)
    out_slot = jnp.where(edge, 1, 0)
    far = lax.rem(yl + 2, 4)

    def products(rows, j):
        wide = [
            jnp.dot(
                rows, wb[:, pl.ds(pl.multiple_of(base + j * CW, CW), CW)],
                preferred_element_type=F32,
            )
            for base in (0, HALF)
        ]
        pieces = []
        for d in range(rows.shape[0] // UNIT):
            cores = [
                jnp.concatenate(
                    [a[d * UNIT + k * ROWS:d * UNIT + (k + 1) * ROWS] for a in wide], axis=0
                )
                for k in range(2)
            ]
            pieces.append(
                (jnp.where(c == 0, cores[0], cores[1]), jnp.where(c == 0, cores[1], cores[0]))
            )
        return pieces

    def project(j):
        for d, (mine, theirs) in enumerate(products(ctx[...], j)):
            own[d, j] = mine
            psend[j, d] = theirs.astype(BF16)
        partner_copy(j).start()

    def combine(j):
        partner_copy(j).wait_recv()
        for d in range(4):
            own[d, j] = own[d, j] + precv[j, d].astype(F32)
        sbuf[0, j] = own[far, j].astype(BF16)
        send(0, j, first_slot, inward).start()

    project(0)

    @pl.loop(1, NC)
    def _(j):
        project(j)
        combine(j - 1)

    combine(NC - 1)

    @pl.when(edge)
    def _():
        @pl.loop(0, NC)
        def _(j):
            sbuf[1, j] = own[yl_in, j].astype(BF16)
            send(1, j, second_slot, inward).start()

        swap.wait_recv()

        def project_x(j):
            ((mine, theirs),) = products(ctxx[...], j)
            ownx[j] = mine
            psendx[j] = theirs.astype(BF16)
            partner_copy_x(j).start()

        def combine_x(j):
            partner_copy_x(j).wait_recv()
            sbuf[2, j] = (ownx[j] + precvx[j].astype(F32)).astype(BF16)
            send(2, j, out_slot, outward).start()

        project_x(0)

        @pl.loop(1, NC)
        def _(j):
            project_x(j)
            combine_x(j - 1)

        combine_x(NC - 1)

    @pl.when(jnp.logical_not(edge))
    def _():
        @pl.loop(0, NC)
        def _(j):
            send(0, j, 2, inward).wait_recv()
            sbuf[2, j] = (own[yl_out, j] + rbuf[2, j].astype(F32)).astype(BF16)
            send(2, j, out_slot, outward).start()
            send(0, j, 0, inward).wait_recv()
            sbuf[1, j] = (own[yl_in, j] + rbuf[0, j].astype(F32)).astype(BF16)
            send(1, j, second_slot, inward).start()

    last_a = jnp.where(edge, 0, 1)
    last_b = jnp.where(edge, 1, 3)

    @pl.loop(0, NC)
    def _(j):
        send(0, j, last_a, inward).wait_recv()
        send(0, j, last_b, inward).wait_recv()
        total = own[yl, j] + rbuf[last_a, j].astype(F32) + rbuf[last_b, j].astype(F32)
        total = total.astype(BF16)
        out_ref[:, pl.ds(pl.multiple_of(j * CW, CW), CW)] = total[:ROWS]
        out_ref[:, pl.ds(pl.multiple_of(HALF + j * CW, CW), CW)] = total[ROWS:]

    for part in range(PARTS):
        def sent(sem, part=part):
            kv_copy(0, 0, part, sem, left).wait_send()

        for d in (1, 2, 3, 4):
            pl.when(((x < 7) & (d - 1 <= s)) | ((x == 7) & (d + 7 <= s)))(
                functools.partial(sent, d)
            )
        for d in (5, 6, 7):
            pl.when((x >= 1) & (x <= d) & (d + 1 <= s))(functools.partial(sent, d))
            if d == 5:
                pl.when((x >= 4) & (x <= 6) & (s >= 4))(functools.partial(sent, 13))
            else:
                pl.when(x + d <= 7)(functools.partial(sent, d + 8))
        pl.when(s < 120)(functools.partial(sent, 8))
        for d in (9, 10, 11, 12):
            up_goes = jnp.logical_not(last_z) & (d - 8 <= s)
            up_goes = up_goes | (across & (d - 8 > jnp.maximum(x, 1 - x)))
            pl.when(up_goes)(functools.partial(sent, d))
            late = first_z & (s >= 64)
            if d >= 10:
                late = late & (x < 7) & (x >= d - 9)
            pl.when(late)(functools.partial(sent, d + 8))
        pl.when(far_source)(functools.partial(sent, 16))

    @pl.loop(0, NC)
    def _(j):
        partner_copy(j).wait_send()
        send(0, j, first_slot, inward).wait_send()
        send(1, j, second_slot, inward).wait_send()
        send(2, j, out_slot, outward).wait_send()

    @pl.when(edge)
    def _():
        swap.wait_send()

        @pl.loop(0, NC)
        def _(j):
            partner_copy_x(j).wait_send()


def per_device(query_rows, key_rows, value_rows, document_ids, output_weight):
    any_space = pl.BlockSpec(memory_space=pl.ANY)
    vmem = pl.BlockSpec(memory_space=pltpu.VMEM)
    dma = pltpu.SemaphoreType.DMA
    return pl.pallas_call(
        kernel,
        out_shape=pltpu.VMEM((ROWS, 2 * HALF), BF16),
        in_specs=[any_space, any_space, any_space, vmem, any_space],
        out_specs=vmem,
        scratch_shapes=[
            pltpu.VMEM((SLOTS, PARTS, PIECE, HD), BF16),
            pltpu.VMEM((L, HD), BF16),
            pltpu.VMEM((G * HD, 2 * HALF), BF16),
            pltpu.VMEM((1, L), jnp.int32),
            pltpu.VMEM((1, L), F32),
            pltpu.VMEM((1, L), F32),
            pltpu.VMEM((HD, L), F32),
            pltpu.VMEM((T, G * HD), BF16),
            pltpu.VMEM((UNIT, G * HD), BF16),
            pltpu.VMEM((4, NC, UNIT, CW), F32),
            pltpu.VMEM((NC, 4, UNIT, CW), BF16),
            pltpu.VMEM((NC, 4, UNIT, CW), BF16),
            pltpu.VMEM((NC, UNIT, CW), F32),
            pltpu.VMEM((NC, UNIT, CW), BF16),
            pltpu.VMEM((NC, UNIT, CW), BF16),
            pltpu.VMEM((3, NC, UNIT, CW), BF16),
            pltpu.VMEM((4, NC, UNIT, CW), BF16),
            dma((G + PARTS,)),
            dma,
            dma((21, PARTS)),
            dma((SLOTS, PARTS)),
            dma((2,)),
            dma((2, NC)),
            dma((2, NC)),
            dma((3, NC)),
            dma((4, NC)),
        ],
        compiler_params=pltpu.CompilerParams(
            collective_id=0, has_side_effects=True, vmem_limit_bytes=56 * 1024 * 1024
        ),
        name="attend_project",
    )(query_rows, key_rows, value_rows, document_ids.reshape(T, HD), output_weight)


def solution(mesh):
    in_specs = (P("seq", "tp"), P("seq", "tp"), P("seq", "tp"), P(), P("tp", None))
    out_specs = P(("seq", "tp"), None)
    return jax.shard_map(
        per_device, mesh=mesh, in_specs=in_specs, out_specs=out_specs, check_vma=False
    )
```

```python
import functools
import math

import jax
import jax.numpy as jnp
from jax import lax
from jax.experimental import pallas as pl
from jax.experimental.pallas import tpu as pltpu
from jax.sharding import PartitionSpec as P

MESH = pl.DeviceIdType.MESH
F32 = jnp.float32
BF16 = jnp.bfloat16

T = 192
HD = 128
G = 4
L = G * T
BACK = 12
NC = 4
CW = 1024
HALF = 4096
ROWS = 24
UNIT = 2 * ROWS
NEG = -1e30
PARTS = 2
PIECE = T
SLOTS = 17
TAIL = (9, 10, 11, 12)
ORDER = [(8, 1, 7, 2, 6, 3, 5, 4) + TAIL]
ORDER += [(1, 8, 2, 7, 3, 6, 4, 5) + TAIL] * 6
ORDER += [(1, 8, 2, 9, 3, 10, 4, 11, 7, 6, 5, 12)]
ORDER_Z0 = [
    (8, 1, 7, 2, 6, 9, 3, 5, 10, 4, 11, 12),
    (1, 8, 7, 9, 2, 6, 10, 3, 5, 4, 11, 12),
    (1, 2, 8, 9, 7, 10, 6, 3, 5, 11, 4, 12),
    (1, 2, 3, 8, 9, 7, 10, 6, 11, 5, 4, 12),
    (1, 2, 3, 4, 8, 9, 7, 10, 6, 11, 5, 12),
    (1, 2, 3, 4, 5, 8, 9, 7, 10, 6, 11, 12),
    (1, 2, 3, 4, 6, 5, 8, 9, 7, 10, 11, 12),
    (1, 2, 3, 4, 7, 6, 5, 8, 16, 9, 10, 11, 12),
]
SCALE = math.log2(math.e) / math.sqrt(HD)
LT = 384
WORD = 6
WORDS = 3


def packed(order):
    order = tuple(order) + (0,) * (WORD * WORDS - len(order))
    return [
        sum(d << (5 * n) for n, d in enumerate(order[w * WORD:(w + 1) * WORD]))
        for w in range(WORDS)
    ]


def kernel(
    q_hbm, k_hbm, v_hbm, doc_ref, w_hbm, out_ref,
    kvb, qb, wb, start_ref, max_ref, sum_ref, acc, ctx, ctxx,
    own, psend, precv, ownx, psendx, precvx, sbuf, rbuf,
    lsem, wsem, kvsend, kvrecv, csem, psem, pxsem, ssem, rsem,
):
    s = lax.axis_index("seq")
    t = lax.axis_index("tp")
    x = lax.rem(s, 8)
    row = s - x
    yl = t // 2
    c = lax.rem(t, 2)
    other = lax.rem(s + 64, 128)
    first_z = lax.rem(s, 64) < 8
    last_z = lax.rem(s, 64) >= 56
    across = (s >= 56) & (s < 64) & (x < 4)
    far_source = s == 55
    far_target = s == 71
    edge = (yl == 0) | (yl == 3)

    def in_row(step):
        return row + lax.rem(x + step + 8, 8)

    right = (in_row(1), t)
    left = (in_row(-1), t)
    up = (lax.rem(s + 8, 128), t)
    peer = (other, t)
    twin = (s, t + 1 - 2 * c)
    yl_in = jnp.where(yl < 2, yl + 1, yl - 1)
    yl_out = jnp.where((yl == 0) | (yl == 2), 3, 0)
    inward = (s, 2 * yl_in + c)
    outward = (jnp.where(edge, other, s), 2 * yl_out + c)

    q_copies = [
        pltpu.make_async_copy(
            q_hbm.at[:, pl.ds(h * HD, HD)], qb.at[pl.ds(h * T, T), :], lsem.at[h]
        )
        for h in range(G)
    ]
    kv_loads = [
        pltpu.make_async_copy(
            (k_hbm, v_hbm)[i], kvb.at[0, i], lsem.at[G + i],
        )
        for i in range(PARTS)
    ]
    w_copy = pltpu.make_async_copy(w_hbm, wb, wsem)
    for copy in kv_loads:
        copy.start()
    for copy in q_copies:
        copy.start()
    w_copy.start()

    barrier = pltpu.get_barrier_semaphore()
    friends = [(in_row(m), t) for m in (1, 2, -1, -2)]
    friends += [(lax.rem(s + 120, 128), t), peer, twin, inward, outward]
    for friend in friends:
        pl.semaphore_signal(barrier, inc=1, device_id=friend, device_id_type=MESH)
    far_signal = (lax.rem(s + 112, 128), t)

    @pl.when(far_target)
    def _():
        pl.semaphore_signal(barrier, inc=1, device_id=far_signal, device_id_type=MESH)

    pl.semaphore_wait(barrier, len(friends) + jnp.where(far_source, 1, 0))

    def kv_copy(src, dst, part, sem, device):
        return pltpu.make_async_remote_copy(
            src_ref=kvb.at[src, part], dst_ref=kvb.at[dst, part],
            send_sem=kvsend.at[sem, part], recv_sem=kvrecv.at[dst, part],
            device_id=device, device_id_type=MESH,
        )

    def right_sem(to):
        return jnp.where(to <= 4, to, to + 8)

    def forward(d, part):
        middle = (d >= 8) & (d <= 11)
        passing = d >= 16

        @pl.when(((x < 7) & ((d <= 3) | ((d == 4) & (x >= 4)) | (first_z & middle & (d <= x + 8)))) | ((x == 7) & (middle | passing)))
        def _():
            to = jnp.where(x < 7, d + 1, d - 7)
            kv_copy(d, to, part, right_sem(to), right).start()

        @pl.when(((d <= 4) & jnp.logical_not(last_z)) | (across & (d <= 4) & (d > jnp.maximum(x, 1 - x))))
        def _():
            kv_copy(d, d + 8, part, d + 8, up).start()

        @pl.when((d >= 6) & (d <= 8) & (x >= 1) & (x <= d - 1))
        def _():
            kv_copy(d, d - 1, part, d - 1, left).start()

    def direct(e):
        @pl.when(x + e <= 7)
        def _():
            for part in range(PARTS):
                kv_copy(0, e, part, e + 8, (s + e, t)).start()

    for part, copy in enumerate(kv_loads):
        copy.wait()

        @pl.when(x < 7)
        def _(part=part):
            kv_copy(0, 1, part, 1, right).start()

        @pl.when(s < 120)
        def _(part=part):
            kv_copy(0, 8, part, 8, up).start()

        @pl.when(far_source)
        def _(part=part):
            kv_copy(0, 16, part, 16, (s + 16, t)).start()

    direct(7)

    @pl.when(first_z)
    def _():
        direct(6)

    first = (3 * s) // 2
    odd = lax.rem(s, 2)

    def column(r):
        vals = doc_ref[pl.ds(r, 1), :].astype(F32)
        return jnp.transpose(jnp.broadcast_to(vals, (HD, HD)))

    two = jnp.concatenate([column(first), column(first + 1)], axis=0)
    qdoc = jnp.where(odd == 0, two[:T], two[HD // 2:HD // 2 + T])
    span = 21
    low = jnp.clip(first - 18, 0, T - span)

    def count(n, total):
        vals = doc_ref[pl.ds(low + n, 1), :].astype(F32)
        return total + jnp.where(vals < qdoc, 1.0, 0.0)

    counted = lax.fori_loop(0, span, count, jnp.zeros((T, HD), F32))
    counted = jnp.transpose(jnp.concatenate([counted] * G, axis=0))
    begin = jnp.sum(counted, axis=0, keepdims=True).astype(jnp.int32)
    start_ref[...] = begin + (low * HD - s * T)

    for copy in q_copies:
        copy.wait()

    max_ref[...] = jnp.full((1, L), NEG, F32)
    sum_ref[...] = jnp.zeros((1, L), F32)
    acc[...] = jnp.zeros((HD, L), F32)

    def attend(d, diagonal=False):
        keys = kvb[d, 0]
        values = kvb[d, 1]
        for n in range(L // LT):
            cols = pl.ds(n * LT, LT)
            scores = lax.dot_general(
                keys, qb[cols, :], (((1,), (1,)), ((), ())), preferred_element_type=F32
            )
            pos = lax.broadcasted_iota(jnp.int32, (T, LT), 0)
            allowed = pos >= start_ref[:, cols] + d * T
            if diagonal:
                lane = n * LT + lax.broadcasted_iota(jnp.int32, (1, LT), 1)
                query = lane
                for h in range(1, G):
                    query = jnp.where(lane >= h * T, lane - h * T, query)
                allowed = allowed & (pos <= query)
            scores = jnp.where(allowed, scores * SCALE, NEG)
            old = max_ref[:, cols]
            new = jnp.maximum(old, jnp.max(scores, axis=0, keepdims=True))
            expo = jnp.exp2(scores - new)
            alpha = jnp.exp2(old - new)
            max_ref[:, cols] = new
            sum_ref[:, cols] = sum_ref[:, cols] * alpha + jnp.sum(expo, axis=0, keepdims=True)
            added = lax.dot_general(
                values, expo.astype(BF16), (((0,), (0,)), ((), ())), preferred_element_type=F32
            )
            acc[:, cols] = acc[:, cols] * alpha + added

    attend(0, True)

    def order(index):
        word = 0
        for table, is_z0 in ((ORDER, False), (ORDER_Z0, True)):
            for place in range(8):
                here = (x == place) & (first_z if is_z0 else jnp.logical_not(first_z))
                word = jnp.where(here, packed(table[place])[index], word)
        return word

    words = [order(index) for index in range(WORDS)]

    @pl.loop(0, WORD * WORDS)
    def _(n):
        word = jnp.where(n < WORD, words[0], jnp.where(n < 2 * WORD, words[1], words[2]))
        d = lax.shift_right_logical(word, 5 * lax.rem(n, WORD)) & 31
        there = (d > 0) & (d <= s)

        @pl.when(there)
        def _():
            for part in range(PARTS):
                kv_copy(d, d, part, d, left).wait_recv()
                forward(d, part)

        @pl.when((n == 1) & jnp.logical_not(first_z))
        def _():
            direct(6)

        @pl.when(there & (d <= BACK))
        def _():
            attend(d)

    done = jnp.transpose(acc[...] / sum_ref[...])
    for h in range(G):
        ctx[:, h * HD:(h + 1) * HD] = done[h * T:(h + 1) * T].astype(BF16)

    swap = pltpu.make_async_remote_copy(
        src_ref=ctx.at[pl.ds(pl.multiple_of(UNIT * yl_out, 16), UNIT), :], dst_ref=ctxx,
        send_sem=csem.at[0], recv_sem=csem.at[1], device_id=peer, device_id_type=MESH,
    )

    @pl.when(edge)
    def _():
        swap.start()

    w_copy.wait()

    def partner_copy(j):
        return pltpu.make_async_remote_copy(
            src_ref=psend.at[j], dst_ref=precv.at[j],
            send_sem=psem.at[0, j], recv_sem=psem.at[1, j],
            device_id=twin, device_id_type=MESH,
        )

    def partner_copy_x(j):
        return pltpu.make_async_remote_copy(
            src_ref=psendx.at[j], dst_ref=precvx.at[j],
            send_sem=pxsem.at[0, j], recv_sem=pxsem.at[1, j],
            device_id=twin, device_id_type=MESH,
        )

    def send(kind, j, slot, device):
        return pltpu.make_async_remote_copy(
            src_ref=sbuf.at[kind, j], dst_ref=rbuf.at[slot, j],
            send_sem=ssem.at[kind, j], recv_sem=rsem.at[slot, j],
            device_id=device, device_id_type=MESH,
        )

    first_slot = jnp.where(edge, 0, 2)
    second_slot = jnp.where(edge, 1, 3)
    out_slot = jnp.where(edge, 1, 0)
    far = lax.rem(yl + 2, 4)

    def products(rows, j):
        wide = [
            jnp.dot(
                rows, wb[:, pl.ds(pl.multiple_of(base + j * CW, CW), CW)],
                preferred_element_type=F32,
            )
            for base in (0, HALF)
        ]
        pieces = []
        for d in range(rows.shape[0] // UNIT):
            cores = [
                jnp.concatenate(
                    [a[d * UNIT + k * ROWS:d * UNIT + (k + 1) * ROWS] for a in wide], axis=0
                )
                for k in range(2)
            ]
            pieces.append(
                (jnp.where(c == 0, cores[0], cores[1]), jnp.where(c == 0, cores[1], cores[0]))
            )
        return pieces

    def project(j):
        for d, (mine, theirs) in enumerate(products(ctx[...], j)):
            own[d, j] = mine
            psend[j, d] = theirs.astype(BF16)
        partner_copy(j).start()

    def combine(j):
        partner_copy(j).wait_recv()
        for d in range(4):
            own[d, j] = own[d, j] + precv[j, d].astype(F32)
        sbuf[0, j] = own[far, j].astype(BF16)
        send(0, j, first_slot, inward).start()

    project(0)

    @pl.loop(1, NC)
    def _(j):
        project(j)
        combine(j - 1)

    combine(NC - 1)

    @pl.when(edge)
    def _():
        @pl.loop(0, NC)
        def _(j):
            sbuf[1, j] = own[yl_in, j].astype(BF16)
            send(1, j, second_slot, inward).start()

        swap.wait_recv()

        def project_x(j):
            ((mine, theirs),) = products(ctxx[...], j)
            ownx[j] = mine
            psendx[j] = theirs.astype(BF16)
            partner_copy_x(j).start()

        def combine_x(j):
            partner_copy_x(j).wait_recv()
            sbuf[2, j] = (ownx[j] + precvx[j].astype(F32)).astype(BF16)
            send(2, j, out_slot, outward).start()

        project_x(0)

        @pl.loop(1, NC)
        def _(j):
            project_x(j)
            combine_x(j - 1)

        combine_x(NC - 1)

    @pl.when(jnp.logical_not(edge))
    def _():
        @pl.loop(0, NC)
        def _(j):
            send(0, j, 2, inward).wait_recv()
            sbuf[2, j] = (own[yl_out, j] + rbuf[2, j].astype(F32)).astype(BF16)
            send(2, j, out_slot, outward).start()
            send(0, j, 0, inward).wait_recv()
            sbuf[1, j] = (own[yl_in, j] + rbuf[0, j].astype(F32)).astype(BF16)
            send(1, j, second_slot, inward).start()

    last_a = jnp.where(edge, 0, 1)
    last_b = jnp.where(edge, 1, 3)

    @pl.loop(0, NC)
    def _(j):
        send(0, j, last_a, inward).wait_recv()
        send(0, j, last_b, inward).wait_recv()
        total = own[yl, j] + rbuf[last_a, j].astype(F32) + rbuf[last_b, j].astype(F32)
        total = total.astype(BF16)
        out_ref[:, pl.ds(pl.multiple_of(j * CW, CW), CW)] = total[:ROWS]
        out_ref[:, pl.ds(pl.multiple_of(HALF + j * CW, CW), CW)] = total[ROWS:]

    for part in range(PARTS):
        def sent(sem, part=part):
            kv_copy(0, 0, part, sem, left).wait_send()

        for d in (1, 2, 3, 4):
            pl.when(((x < 7) & (d - 1 <= s)) | ((x == 7) & (d + 7 <= s)))(
                functools.partial(sent, d)
            )
        for d in (5, 6, 7):
            pl.when((x >= 1) & (x <= d) & (d + 1 <= s))(functools.partial(sent, d))
            if d == 5:
                pl.when((x >= 4) & (x <= 6) & (s >= 4))(functools.partial(sent, 13))
            else:
                pl.when(x + d <= 7)(functools.partial(sent, d + 8))
        pl.when(s < 120)(functools.partial(sent, 8))
        for d in (9, 10, 11, 12):
            up_goes = jnp.logical_not(last_z) & (d - 8 <= s)
            up_goes = up_goes | (across & (d - 8 > jnp.maximum(x, 1 - x)))
            pl.when(up_goes)(functools.partial(sent, d))
            late = first_z & (s >= 64)
            if d >= 10:
                late = late & (x < 7) & (x >= d - 9)
            pl.when(late)(functools.partial(sent, d + 8))
        pl.when(far_source)(functools.partial(sent, 16))

    @pl.loop(0, NC)
    def _(j):
        partner_copy(j).wait_send()
        send(0, j, first_slot, inward).wait_send()
        send(1, j, second_slot, inward).wait_send()
        send(2, j, out_slot, outward).wait_send()

    @pl.when(edge)
    def _():
        swap.wait_send()

        @pl.loop(0, NC)
        def _(j):
            partner_copy_x(j).wait_send()


def per_device(query_rows, key_rows, value_rows, document_ids, output_weight):
    any_space = pl.BlockSpec(memory_space=pl.ANY)
    vmem = pl.BlockSpec(memory_space=pltpu.VMEM)
    dma = pltpu.SemaphoreType.DMA
    return pl.pallas_call(
        kernel,
        out_shape=pltpu.VMEM((ROWS, 2 * HALF), BF16),
        in_specs=[any_space, any_space, any_space, vmem, any_space],
        out_specs=vmem,
        scratch_shapes=[
            pltpu.VMEM((SLOTS, PARTS, PIECE, HD), BF16),
            pltpu.VMEM((L, HD), BF16),
            pltpu.VMEM((G * HD, 2 * HALF), BF16),
            pltpu.VMEM((1, L), jnp.int32),
            pltpu.VMEM((1, L), F32),
            pltpu.VMEM((1, L), F32),
            pltpu.VMEM((HD, L), F32),
            pltpu.VMEM((T, G * HD), BF16),
            pltpu.VMEM((UNIT, G * HD), BF16),
            pltpu.VMEM((4, NC, UNIT, CW), F32),
            pltpu.VMEM((NC, 4, UNIT, CW), BF16),
            pltpu.VMEM((NC, 4, UNIT, CW), BF16),
            pltpu.VMEM((NC, UNIT, CW), F32),
            pltpu.VMEM((NC, UNIT, CW), BF16),
            pltpu.VMEM((NC, UNIT, CW), BF16),
            pltpu.VMEM((3, NC, UNIT, CW), BF16),
            pltpu.VMEM((4, NC, UNIT, CW), BF16),
            dma((G + PARTS,)),
            dma,
            dma((21, PARTS)),
            dma((SLOTS, PARTS)),
            dma((2,)),
            dma((2, NC)),
            dma((2, NC)),
            dma((3, NC)),
            dma((4, NC)),
        ],
        compiler_params=pltpu.CompilerParams(
            collective_id=0, has_side_effects=True, vmem_limit_bytes=56 * 1024 * 1024
        ),
        name="attend_project",
    )(query_rows, key_rows, value_rows, document_ids.reshape(T, HD), output_weight)


def solution(mesh):
    in_specs = (P("seq", "tp"), P("seq", "tp"), P("seq", "tp"), P(), P("tp", None))
    out_specs = P(("seq", "tp"), None)
    return jax.shard_map(
        per_device, mesh=mesh, in_specs=in_specs, out_specs=out_specs, check_vma=False
    )
```
